512 devices in a mesh: grp: 2 (over y), seq: 16 (over z), head: 8 (over x), rep: 2 (over core).
Axes of the slice: x: 8, y: 2, z: 16, core: 2. Of those that a mesh axis runs over, the one named last changes fastest.
The devices are a block of a 8x8x16 slice.
Arguments:
- queries: bfloat16 [16, 4096], P(('grp', 'rep'), 'head'), parts along dimension 0, may hold values from -6 to 6
- k_cache: bfloat16 [16, 16, 16384, 128], P(('grp', 'rep'), 'head', 'seq'), parts along dimension 0, may hold values from -6 to 6
- v_cache: bfloat16 [16, 16, 16384, 128], P(('grp', 'rep'), 'head', 'seq'), parts along dimension 0, may hold values from -6 to 6
- page_table: int32 [16, 128], P(('grp', 'rep')), parts along dimension 0, may hold values from 0 to 127, each once within a row
- lengths: int32 [16], P(('grp', 'rep')), parts along dimension 0, may hold values from 2048 to 16384
- keep_threshold: int32 [16, 16], P(('grp', 'rep'), 'head'), parts along dimension 0, may hold values from 256 to 8191
Outputs:
- attended: bfloat16 [16, 4096], P(('grp', 'rep'), 'head'), parts along dimension 0
- token_mass: float32 [16, 16, 16384], P(('grp', 'rep'), 'head', 'seq'), parts along dimension 0
- page_keep: float32 [16, 16, 128], P(('grp', 'rep'), 'head', 'seq'), parts along dimension 0
The draws below stay inside these ranges and needn't reach their ends.
There are 2 independent parts, one for each index of `grp`. The reference program is written for one: setup_inputs(seed, part) draws one part's arguments, and reference() takes and returns one part's arrays. A program takes and returns all parts, laid end to end along the dimension named above; each array names one. Nothing has to cross between parts.
Inputs may be any that keep to these rules, and one draw needn't show every extreme that they name: `page_table`: each row names every physical page slot 0 to 127 once.
All inputs are finite; a program needn't handle non-finite values.
Results may differ from the reference program's by a relative error of at most 0.0052.
Values sent between devices are 32-bit elements; how exact they have to be, the bound alone decides.
A program may use at most 64 MiB of HBM per device.

```python
import jax
import jax.numpy as jnp
from jax import lax

QH = 32
KVH = 16
HD = 128
PAGE = 128
BATCH = 8
PAGES = 128
CTX = 16384


def set_ends(drawn, own_key, smallest, top_value):
    index_at = [jax.random.randint(jax.random.fold_in(own_key, axis), (), 0, length) for axis, length in enumerate(drawn.shape)]
    longest = drawn.shape.index(max(drawn.shape))
    neighbour = index_at[:longest] + [(index_at[longest] + 1) % drawn.shape[longest]] + index_at[longest + 1:]
    return drawn.at[tuple(index_at)].set(smallest).at[tuple(neighbour)].set(top_value)


def block_levels(rng, extent, shards, smallest, top_value):
    def one(dim, blocks):
        steps = jax.random.uniform(jax.random.fold_in(jax.random.fold_in(rng, 6), dim), (blocks,), jnp.float32, smallest / len(shards), top_value / len(shards))
        return jnp.repeat(jnp.exp(steps), extent[dim] // blocks).reshape((-1,) + (1,) * (len(extent) - dim - 1))

    gain = one(*shards[0])
    for cut in shards[1:]:
        gain = gain * one(*cut)
    return gain


def centred(own_key, shape, scale, bound, cuts=(), kind=jnp.bfloat16):
    gain = block_levels(own_key, shape, cuts, -0.22, 0.18) if cuts else 1.0
    result = jax.random.normal(own_key, shape, jnp.float32) * scale * gain
    return jnp.minimum(jnp.maximum(result, -bound), bound).astype(kind)


def setup_inputs(seed: int = 0, part: int = 0) -> dict:
    arg_keys = jax.random.split(jax.random.key(seed), 7)
    part_splits = jax.random.split(jax.random.fold_in(arg_keys[6], part), 7)
    return {
        "queries": centred(part_splits[0], (BATCH, QH * HD), 1.0, 6.0, ((0, 2), (1, 8))),
        "k_cache": centred(part_splits[1], (BATCH, KVH, CTX, HD), 1.0, 6.0, ((0, 2), (1, 8), (2, 16))),
        "v_cache": centred(part_splits[2], (BATCH, KVH, CTX, HD), 1.0, 6.0, ((0, 2), (1, 8), (2, 16))),
        "page_table": jax.vmap(lambda own: jax.random.permutation(own, PAGES))(jax.random.split(part_splits[3], BATCH)).reshape((BATCH, PAGES)).astype(jnp.int32),
        "lengths": set_ends(jax.random.randint(part_splits[4], (BATCH,), CTX // 8, CTX + 1), jax.random.fold_in(part_splits[4], 1), CTX // 8, CTX).astype(jnp.int32),
        "keep_threshold": set_ends(jax.random.randint(part_splits[5], (BATCH, KVH), 256, 8192), jax.random.fold_in(part_splits[5], 1), 256, 8191).astype(jnp.int32),
    }


softcap = 50.0
query_scale = 1.0 / 12.0
quanta = 65536.0


def one_request(inputs):
    query_row, keys_all, values_all, table_row, length_one, threshold_row = inputs
    group = QH // KVH
    slots = (table_row[:, None] * PAGE + jnp.arange(PAGE, dtype=jnp.int32)[None, :]).reshape(-1).astype(jnp.int32)
    keys_logical = keys_all[:, slots, :].astype(jnp.float32)
    values_logical = values_all[:, slots, :].astype(jnp.float32)
    grouped = query_row.reshape(KVH, group, HD).astype(jnp.float32)
    logits = jnp.einsum("kgd,ktd->kgt", grouped, keys_logical)
    capped = softcap * jnp.tanh(logits * query_scale / softcap)
    is_live = jnp.arange(CTX, dtype=jnp.int32) < length_one
    weights = jnp.where(is_live[None, None, :], jnp.exp(capped - softcap), jnp.float32(0.0))
    denom = jnp.sum(weights, axis=2)
    numer = jnp.einsum("kgt,ktd->kgd", weights.astype(jnp.bfloat16).astype(jnp.float32), values_logical)
    attended = (numer / denom[:, :, None]).astype(jnp.bfloat16).reshape(QH * HD)
    token_mass = jnp.sum(weights / denom[:, :, None], axis=1)
    page_mass = jnp.sum(token_mass.reshape(KVH, PAGES, PAGE), axis=2)
    page_keep = jnp.minimum(jnp.float32(1.0), quanta * page_mass / threshold_row.astype(jnp.float32)[:, None])
    return attended, token_mass, page_keep


def reference(queries, k_cache, v_cache, page_table, lengths, keep_threshold):
    attended, token_mass, page_keep = lax.map(one_request, (queries, k_cache, v_cache, page_table, lengths, keep_threshold))
    return (attended, token_mass, page_keep)
```

```python
import jax
import jax.numpy as jnp
from jax import lax
from jax.experimental import pallas as pl
from jax.experimental.pallas import tpu as pltpu
from jax.sharding import PartitionSpec as P

PAGE = 128
SUBS = 4
MESH = pl.DeviceIdType.MESH

softcap = 50.0
query_scale = 1.0 / 12.0
quanta = 65536.0


def attend(
    q_ref, pt_vec, pt_ref, len_ref, thr_ref, k_hbm, v_hbm,
    att_ref, mass_ref, keep_ref,
    kbuf, vbuf, gath, part, att32, k_sem, v_sem, g_send, g_recv, p_send, p_recv,
):
    n = lax.axis_size("seq")
    z = lax.axis_index("seq")
    requests = k_hbm.shape[0]
    pairs = requests // 2
    slots = k_hbm.shape[2] // PAGE
    per = slots // SUBS

    def ring(step):
        return lax.rem(z + step + 2 * n, n)

    copies = []
    for r in range(requests):
        k_copy = pltpu.make_async_copy(k_hbm.at[r], kbuf.at[r], k_sem.at[r])
        k_copy.start()
        copies.append(k_copy)
    v_copies = []
    for r in range(requests):
        v_copy = pltpu.make_async_copy(v_hbm.at[r], vbuf.at[r], v_sem.at[r])
        v_copy.start()
        v_copies.append(v_copy)
    barrier = pltpu.get_barrier_semaphore()
    for step in (1, -1):
        pl.semaphore_signal(barrier, inc=1, device_id={"seq": ring(step)}, device_id_type=MESH)

    sub = lax.broadcasted_iota(jnp.int32, (8, PAGE), 0)
    lane = lax.broadcasted_iota(jnp.int32, (8, PAGE), 1)
    first = lax.rem(sub, 4) < 2
    queries = q_ref[...].astype(jnp.float32)

    def rows_of(even, odd):
        return jnp.where(first, even, odd)

    weights = []
    denoms = []
    for p in range(pairs):
        logits = None
        for ri in range(2):
            r = 2 * p + ri
            lhs = []
            for kv in range(2):
                row = ri * 2 + kv
                block = jnp.where(
                    sub == row,
                    queries[r : r + 1, (2 * kv) * PAGE : (2 * kv + 1) * PAGE],
                    jnp.where(
                        sub == 4 + row,
                        queries[r : r + 1, (2 * kv + 1) * PAGE : (2 * kv + 2) * PAGE],
                        0.0,
                    ),
                )
                lhs.append(block)
            lhs = jnp.concatenate(lhs, axis=1).astype(jnp.bfloat16)
            copies[r].wait()
            keys = jnp.concatenate([kbuf[r, 0], kbuf[r, 1]], axis=1)
            term = lax.dot_general(
                lhs, keys, (((1,), (1,)), ((), ())), preferred_element_type=jnp.float32
            )
            logits = term if logits is None else logits + term
        table = rows_of(pt_vec[2 * p : 2 * p + 1, :], pt_vec[2 * p + 1 : 2 * p + 2, :])
        length = rows_of(len_ref[2 * p], len_ref[2 * p + 1])
        total = None
        tiles = []
        for s in range(slots):
            hit = jnp.where(table == z * slots + s, lane, 0).astype(jnp.float32)
            logical = jnp.sum(hit, axis=1, keepdims=True).astype(jnp.int32)
            live = logical * PAGE + lane < length
            tile = logits[:, s * PAGE : (s + 1) * PAGE]
            capped = softcap * jnp.tanh(tile * query_scale / softcap)
            tile = jnp.where(live, jnp.exp(capped - softcap), 0.0)
            gath[z * slots + s, p] = tile
            tiles.append(tile)
            total = tile if total is None else total + tile
        weights.append(jnp.concatenate(tiles, axis=1).astype(jnp.bfloat16))
        denoms.append(jnp.sum(total, axis=1, keepdims=True))
    part[z, 2] = jnp.where(lane == 0, denoms[0], denoms[1])

    pl.semaphore_wait(barrier, 2)

    def chunk_copy(src, way, step, c):
        block = gath.at[pl.ds(src * slots + c * per, per)]
        return pltpu.make_async_remote_copy(
            src_ref=block, dst_ref=block,
            send_sem=g_send.at[way, step, c], recv_sem=g_recv.at[way, step, c],
            device_id={"seq": ring(1 - 2 * way)}, device_id_type=MESH,
        )

    def part_copy(src, way, step):
        return pltpu.make_async_remote_copy(
            src_ref=part.at[src], dst_ref=part.at[src],
            send_sem=p_send.at[way, step], recv_sem=p_recv.at[way, step],
            device_id={"seq": ring(1 - 2 * way)}, device_id_type=MESH,
        )

    half = n // 2
    def goes(way, step, c):
        if step < half - 1:
            return True
        return c % 2 == way

    def part_goes(way, step):
        return step < half - 1 or way == 0

    sent = []

    def start(copy):
        copy.start()
        sent.append(copy)

    for c in range(SUBS):
        for way in range(2):
            if goes(way, 0, c):
                start(chunk_copy(z, way, 0, c))

    for p in range(pairs):
        numer = jnp.zeros((8, PAGE), jnp.float32)
        for ri in range(2):
            r = 2 * p + ri
            v_copies[r].wait()
            values = jnp.concatenate([vbuf[r, 0], vbuf[r, 1]], axis=1)
            out = jnp.dot(weights[p], values, preferred_element_type=jnp.float32)
            for kv in range(2):
                mine = lax.rem(sub, 4) == ri * 2 + kv
                numer = jnp.where(mine, out[:, kv * PAGE : (kv + 1) * PAGE], numer)
        part[z, p] = numer
    for way in range(2):
        start(part_copy(z, way, 0))

    for step in range(half):
        for c in range(SUBS):
            for way in range(2):
                if not goes(way, step, c):
                    continue
                src = ring((2 * way - 1) * (step + 1))
                chunk_copy(src, way, step, c).wait_recv()
                if step + 1 < half and goes(way, step + 1, c):
                    start(chunk_copy(src, way, step + 1, c))
        for way in range(2):
            if not part_goes(way, step):
                continue
            src = ring((2 * way - 1) * (step + 1))
            part_copy(src, way, step).wait_recv()
            if step + 1 < half and part_goes(way, step + 1):
                start(part_copy(src, way, step + 1))

    den = jnp.sum(part[:, 2], axis=0)
    for p in range(pairs):
        inv = 1.0 / jnp.sum(jnp.where(lane == p, den, 0.0), axis=1, keepdims=True)
        numer = jnp.sum(part[:, p], axis=0) * inv
        for ri in range(2):
            r = 2 * p + ri
            for kv in range(2):
                for g in range(2):
                    row = g * 4 + ri * 2 + kv
                    h = 2 * kv + g
                    att32[r : r + 1, h * PAGE : (h + 1) * PAGE] = numer[row : row + 1]
        keep = jnp.zeros((4, slots), jnp.float32)
        for j in range(slots):
            even = gath[pt_ref[2 * p, z * slots + j], p]
            odd = gath[pt_ref[2 * p + 1, z * slots + j], p]
            tile = rows_of(even, odd) * inv
            mass = tile[:4] + tile[4:]
            for ri in range(2):
                mass_ref[2 * p + ri, :, j * PAGE : (j + 1) * PAGE] = mass[2 * ri : 2 * ri + 2]
            page = jnp.sum(mass, axis=1, keepdims=True)
            column = lax.broadcasted_iota(jnp.int32, (4, slots), 1)
            keep = jnp.where(column == j, page, keep)
        for ri in range(2):
            r = 2 * p + ri
            which = lax.broadcasted_iota(jnp.int32, (2, slots), 0)
            thr = jnp.where(which == 0, thr_ref[0, r], thr_ref[1, r]).astype(jnp.float32)
            keep_ref[r] = jnp.minimum(1.0, quanta * keep[2 * ri : 2 * ri + 2] / thr)
    att_ref[...] = att32[...].astype(att_ref.dtype)
    for copy in sent:
        copy.wait_send()


def shards(queries, k_cache, v_cache, page_table, lengths, keep_threshold):
    n = lax.axis_size("seq")
    requests, kv_local, tok_local, head_size = k_cache.shape
    slots = tok_local // PAGE
    vmem = pl.BlockSpec(memory_space=pltpu.VMEM)
    smem = pl.BlockSpec(memory_space=pltpu.SMEM)
    hbm = pl.BlockSpec(memory_space=pl.ANY)
    dma = pltpu.SemaphoreType.DMA
    half = n // 2
    return pl.pallas_call(
        attend,
        out_shape=(
            jax.ShapeDtypeStruct(queries.shape, jnp.bfloat16),
            jax.ShapeDtypeStruct((requests, kv_local, tok_local), jnp.float32),
            jax.ShapeDtypeStruct((requests, kv_local, slots), jnp.float32),
        ),
        in_specs=[vmem, vmem, smem, smem, smem, hbm, hbm],
        out_specs=(vmem, vmem, vmem),
        scratch_shapes=[
            pltpu.VMEM(k_cache.shape, k_cache.dtype),
            pltpu.VMEM(v_cache.shape, v_cache.dtype),
            pltpu.VMEM((n * slots, requests // 2, 8, PAGE), jnp.float32),
            pltpu.VMEM((n, 3, 8, PAGE), jnp.float32),
            pltpu.VMEM(queries.shape, jnp.float32),
            dma((requests,)), dma((requests,)),
            dma((2, half, SUBS)), dma((2, half, SUBS)),
            dma((2, half)), dma((2, half)),
        ],
        compiler_params=pltpu.CompilerParams(collective_id=0, has_side_effects=True),
    )(queries, page_table, page_table, lengths, keep_threshold.T, k_cache, v_cache)


def solution(mesh):
    placed = (
        P(("grp", "rep"), "head"),
        P(("grp", "rep"), "head", "seq", None),
        P(("grp", "rep"), "head", "seq", None),
        P(("grp", "rep"), None),
        P(("grp", "rep")),
        P(("grp", "rep"), "head"),
    )
    return jax.shard_map(
        shards,
        mesh=mesh,
        in_specs=placed,
        out_specs=(
            P(("grp", "rep"), "head"),
            P(("grp", "rep"), "head", "seq"),
            P(("grp", "rep"), "head", "seq"),
        ),
        check_vma=False,
    )
```

```python
import jax
import jax.numpy as jnp
from jax import lax
from jax.experimental import pallas as pl
from jax.experimental.pallas import tpu as pltpu
from jax.sharding import PartitionSpec as P

PAGE = 128
CUTS = 2
MESH = pl.DeviceIdType.MESH

softcap = 50.0
query_scale = 1.0 / 12.0
quanta = 65536.0


def attend(
    q_ref, pt_vec, pt_ref, len_ref, thr_ref, k_hbm, v_hbm,
    att_ref, mass_ref, keep_ref,
    kbuf, vbuf, gath, part, att32, k_sem, v_sem,
    g_recv, p_recv, own_send, own_part_send, fwd_send, fwd_part_send, ready,
):
    n = lax.axis_size("seq")
    z = lax.axis_index("seq")
    requests = k_hbm.shape[0]
    pairs = requests // 2
    slots = k_hbm.shape[2] // PAGE
    per = slots // CUTS
    inner = z < n - 1
    after = z > 0

    copies = []
    for r in range(requests):
        k_copy = pltpu.make_async_copy(k_hbm.at[r], kbuf.at[r], k_sem.at[r])
        k_copy.start()
        copies.append(k_copy)
    v_copies = []
    for r in range(requests):
        v_copy = pltpu.make_async_copy(v_hbm.at[r], vbuf.at[r], v_sem.at[r])
        v_copy.start()
        v_copies.append(v_copy)

    barrier = pltpu.get_barrier_semaphore()

    @pl.when(after)
    def _():
        pl.semaphore_wait(barrier, 1)

    @pl.when(inner)
    def _():
        pl.semaphore_signal(barrier, inc=1, device_id={"seq": z + 1}, device_id_type=MESH)

    @pl.when(after)
    def _():
        pl.semaphore_signal(ready, inc=1, device_id={"seq": z - 1}, device_id_type=MESH)

    sub = lax.broadcasted_iota(jnp.int32, (8, PAGE), 0)
    lane = lax.broadcasted_iota(jnp.int32, (8, PAGE), 1)
    first = lax.rem(sub, 4) < 2
    queries = q_ref[...].astype(jnp.float32)

    def rows_of(even, odd):
        return jnp.where(first, even, odd)

    def chunk_copy(src, p, c, send_sem, target):
        block = gath.at[p, pl.ds(src * slots + c * per, per)]
        return pltpu.make_async_remote_copy(
            src_ref=block, dst_ref=block,
            send_sem=send_sem, recv_sem=g_recv.at[src, p, c],
            device_id={"seq": target}, device_id_type=MESH,
        )

    def part_copy(src, send_sem, target):
        return pltpu.make_async_remote_copy(
            src_ref=part.at[src], dst_ref=part.at[src],
            send_sem=send_sem, recv_sem=p_recv.at[src],
            device_id={"seq": target}, device_id_type=MESH,
        )

    weights = []
    denoms = []
    for p in range(pairs):
        logits = None
        for ri in range(2):
            r = 2 * p + ri
            lhs = []
            for kv in range(2):
                row = ri * 2 + kv
                block = jnp.where(
                    sub == row,
                    queries[r : r + 1, (2 * kv) * PAGE : (2 * kv + 1) * PAGE],
                    jnp.where(
                        sub == 4 + row,
                        queries[r : r + 1, (2 * kv + 1) * PAGE : (2 * kv + 2) * PAGE],
                        0.0,
                    ),
                )
                lhs.append(block)
            lhs = jnp.concatenate(lhs, axis=1).astype(jnp.bfloat16)
            copies[r].wait()
            keys = jnp.concatenate([kbuf[r, 0], kbuf[r, 1]], axis=1)
            term = lax.dot_general(
                lhs, keys, (((1,), (1,)), ((), ())), preferred_element_type=jnp.float32
            )
            logits = term if logits is None else logits + term
        table = rows_of(pt_vec[2 * p : 2 * p + 1, :], pt_vec[2 * p + 1 : 2 * p + 2, :])
        length = rows_of(len_ref[2 * p], len_ref[2 * p + 1])
        total = None
        tiles = []
        for s in range(slots):
            hit = jnp.where(table == z * slots + s, lane, 0).astype(jnp.float32)
            logical = jnp.sum(hit, axis=1, keepdims=True).astype(jnp.int32)
            live = logical * PAGE + lane < length
            tile = logits[:, s * PAGE : (s + 1) * PAGE]
            capped = softcap * jnp.tanh(tile * query_scale / softcap)
            tile = jnp.where(live, jnp.exp(capped - softcap), 0.0)
            gath[p, z * slots + s] = tile
            tiles.append(tile)
            total = tile if total is None else total + tile
        weights.append(jnp.concatenate(tiles, axis=1).astype(jnp.bfloat16))
        denoms.append(jnp.sum(total, axis=1, keepdims=True))

        @pl.when(after)
        def _():
            for c in range(CUTS):
                chunk_copy(z, p, c, own_send.at[p, c], 0).start()

    part[z, 2] = jnp.where(lane == 0, denoms[0], denoms[1])
    for p in range(pairs):
        numer = jnp.zeros((8, PAGE), jnp.float32)
        for ri in range(2):
            r = 2 * p + ri
            v_copies[r].wait()
            values = jnp.concatenate([vbuf[r, 0], vbuf[r, 1]], axis=1)
            out = jnp.dot(weights[p], values, preferred_element_type=jnp.float32)
            for kv in range(2):
                mine = lax.rem(sub, 4) == ri * 2 + kv
                numer = jnp.where(mine, out[:, kv * PAGE : (kv + 1) * PAGE], numer)
        part[z, p] = numer

    @pl.when(after)
    def _():
        part_copy(z, own_part_send, 0).start()

    @pl.when(inner)
    def _():
        pl.semaphore_wait(ready, 1)

    def relay(src, carry):
        other = src != z
        passes = jnp.logical_and(inner, src != z + 1)
        for p in range(pairs):
            for c in range(CUTS):

                @pl.when(other)
                def _():
                    chunk_copy(src, p, c, fwd_send.at[src, p, c], 0).wait_recv()

                @pl.when(passes)
                def _():
                    chunk_copy(src, p, c, fwd_send.at[src, p, c], z + 1).start()

        @pl.when(other)
        def _():
            part_copy(src, fwd_part_send.at[src], 0).wait_recv()

        @pl.when(passes)
        def _():
            part_copy(src, fwd_part_send.at[src], z + 1).start()

        return carry

    lax.fori_loop(0, n, relay, 0)

    den = jnp.sum(part[:, 2], axis=0)
    for p in range(pairs):
        inv = 1.0 / jnp.sum(jnp.where(lane == p, den, 0.0), axis=1, keepdims=True)
        numer = jnp.sum(part[:, p], axis=0) * inv
        for ri in range(2):
            r = 2 * p + ri
            for kv in range(2):
                for g in range(2):
                    row = g * 4 + ri * 2 + kv
                    h = 2 * kv + g
                    att32[r : r + 1, h * PAGE : (h + 1) * PAGE] = numer[row : row + 1]
        keep = jnp.zeros((4, slots), jnp.float32)
        for j in range(slots):
            even = gath[p, pt_ref[2 * p, z * slots + j]]
            odd = gath[p, pt_ref[2 * p + 1, z * slots + j]]
            tile = rows_of(even, odd) * inv
            mass = tile[:4] + tile[4:]
            for ri in range(2):
                mass_ref[2 * p + ri, :, j * PAGE : (j + 1) * PAGE] = mass[2 * ri : 2 * ri + 2]
            page = jnp.sum(mass, axis=1, keepdims=True)
            column = lax.broadcasted_iota(jnp.int32, (4, slots), 1)
            keep = jnp.where(column == j, page, keep)
        for ri in range(2):
            r = 2 * p + ri
            which = lax.broadcasted_iota(jnp.int32, (2, slots), 0)
            thr = jnp.where(which == 0, thr_ref[0, r], thr_ref[1, r]).astype(jnp.float32)
            keep_ref[r] = jnp.minimum(1.0, quanta * keep[2 * ri : 2 * ri + 2] / thr)
    att_ref[...] = att32[...].astype(att_ref.dtype)

    @pl.when(after)
    def _():
        for p in range(pairs):
            for c in range(CUTS):
                chunk_copy(z, p, c, own_send.at[p, c], 0).wait_send()
        part_copy(z, own_part_send, 0).wait_send()

    def drain(src, carry):
        @pl.when(jnp.logical_and(inner, src != z + 1))
        def _():
            for p in range(pairs):
                for c in range(CUTS):
                    chunk_copy(src, p, c, fwd_send.at[src, p, c], 0).wait_send()
            part_copy(src, fwd_part_send.at[src], 0).wait_send()

        return carry

    lax.fori_loop(0, n, drain, 0)


def put_out(*refs):
    count = len(refs) // 2
    sems = refs[-1]
    ins, outs = refs[:count], refs[count : 2 * count]
    moves = [pltpu.make_async_copy(i, o, sems.at[k]) for k, (i, o) in enumerate(zip(ins, outs))]
    for move in moves:
        move.start()
    for move in moves:
        move.wait()


def shards(queries, k_cache, v_cache, page_table, lengths, keep_threshold):
    n = lax.axis_size("seq")
    requests, kv_local, tok_local, head_size = k_cache.shape
    slots = tok_local // PAGE
    vmem = pl.BlockSpec(memory_space=pltpu.VMEM)
    smem = pl.BlockSpec(memory_space=pltpu.SMEM)
    hbm = pl.BlockSpec(memory_space=pl.ANY)
    dma = pltpu.SemaphoreType.DMA
    pairs = requests // 2
    results = (
        (queries.shape, jnp.bfloat16),
        ((requests, kv_local, tok_local), jnp.float32),
        ((requests, kv_local, slots), jnp.float32),
    )
    held = pl.pallas_call(
        attend,
        out_shape=tuple(pltpu.VMEM(*result) for result in results),
        in_specs=[vmem, vmem, smem, smem, smem, hbm, hbm],
        out_specs=(vmem, vmem, vmem),
        scratch_shapes=[
            pltpu.VMEM(k_cache.shape, k_cache.dtype),
            pltpu.VMEM(v_cache.shape, v_cache.dtype),
            pltpu.VMEM((pairs, n * slots, 8, PAGE), jnp.float32),
            pltpu.VMEM((n, 3, 8, PAGE), jnp.float32),
            pltpu.VMEM(queries.shape, jnp.float32),
            dma((requests,)), dma((requests,)),
            dma((n, pairs, CUTS)), dma((n,)),
            dma((pairs, CUTS)), dma,
            dma((n, pairs, CUTS)), dma((n,)),
            pltpu.SemaphoreType.REGULAR,
        ],
        compiler_params=pltpu.CompilerParams(collective_id=0, has_side_effects=True),
    )(queries, page_table, page_table, lengths, keep_threshold.T, k_cache, v_cache)
    return pl.pallas_call(
        put_out,
        out_shape=tuple(jax.ShapeDtypeStruct(*result) for result in results),
        in_specs=[vmem] * 3,
        out_specs=(hbm, hbm, hbm),
        scratch_shapes=[dma((3,))],
    )(*(pltpu.with_memory_space_constraint(h, pltpu.VMEM) for h in held))


def solution(mesh):
    placed = (
        P(("grp", "rep"), "head"),
        P(("grp", "rep"), "head", "seq", None),
        P(("grp", "rep"), "head", "seq", None),
        P(("grp", "rep"), None),
        P(("grp", "rep")),
        P(("grp", "rep"), "head"),
    )
    return jax.shard_map(
        shards,
        mesh=mesh,
        in_specs=placed,
        out_specs=(
            P(("grp", "rep"), "head"),
            P(("grp", "rep"), "head", "seq"),
            P(("grp", "rep"), "head", "seq"),
        ),
        check_vma=False,
    )
```

```python
import jax
import jax.numpy as jnp
from jax import lax
from jax.experimental import pallas as pl
from jax.experimental.pallas import tpu as pltpu
from jax.sharding import PartitionSpec as P

PAGE = 128
CUTS = 2
TAIL = 2
MESH = pl.DeviceIdType.MESH

softcap = 50.0
query_scale = 1.0 / 12.0
quanta = 65536.0


def attend(
    q_ref, pt_vec, pt_ref, len_ref, thr_ref, k_hbm, v_hbm,
    att_ref, mass_ref, keep_ref,
    kbuf, vbuf, gath, part, att32, k_sem, v_sem,
    g_recv, p_recv, own_send, own_part_send, fwd_send, fwd_part_send, zero_send, zero_part_send,
    ready, zero_ready,
):
    n = lax.axis_size("seq")
    z = lax.axis_index("seq")
    requests = k_hbm.shape[0]
    pairs = requests // 2
    slots = k_hbm.shape[2] // PAGE
    per = slots // CUTS
    edge = z == 0
    hub = z == 1
    follows = z > 1
    passes_on = jnp.logical_and(z > 0, z < n - 1)

    copies = []
    for r in range(requests):
        k_copy = pltpu.make_async_copy(k_hbm.at[r], kbuf.at[r], k_sem.at[r])
        k_copy.start()
        copies.append(k_copy)
    v_copies = []
    for r in range(requests):
        v_copy = pltpu.make_async_copy(v_hbm.at[r], vbuf.at[r], v_sem.at[r])
        v_copy.start()
        v_copies.append(v_copy)

    barrier = pltpu.get_barrier_semaphore()

    def greet(target):
        pl.semaphore_signal(barrier, inc=1, device_id={"seq": target}, device_id_type=MESH)

    @pl.when(hub)
    def _():
        greet(0)
        for other in range(2, n - TAIL):
            greet(other)

    @pl.when(edge)
    def _():
        for other in range(n - TAIL, n):
            greet(other)

    @pl.when(passes_on)
    def _():
        greet(z + 1)

    sub = lax.broadcasted_iota(jnp.int32, (8, PAGE), 0)
    lane = lax.broadcasted_iota(jnp.int32, (8, PAGE), 1)
    first = lax.rem(sub, 4) < 2
    queries = q_ref[...].astype(jnp.float32)

    def rows_of(even, odd):
        return jnp.where(first, even, odd)

    def chunk_copy(src, p, c, send_sem, target):
        block = gath.at[p, pl.ds(src * slots + c * per, per)]
        return pltpu.make_async_remote_copy(
            src_ref=block, dst_ref=block,
            send_sem=send_sem, recv_sem=g_recv.at[src, p, c],
            device_id={"seq": target}, device_id_type=MESH,
        )

    def part_copy(src, send_sem, target):
        return pltpu.make_async_remote_copy(
            src_ref=part.at[src], dst_ref=part.at[src],
            send_sem=send_sem, recv_sem=p_recv.at[src],
            device_id={"seq": target}, device_id_type=MESH,
        )

    direct = jnp.logical_or(edge, follows)
    target = jnp.where(jnp.logical_or(edge, z < n - TAIL), 1, 0)

    def greeted():
        @pl.when(edge)
        def _():
            pl.semaphore_wait(barrier, 1)
            pl.semaphore_signal(zero_ready, inc=1, device_id={"seq": 1}, device_id_type=MESH)

        @pl.when(follows)
        def _():
            pl.semaphore_wait(barrier, 2)
            pl.semaphore_signal(ready, inc=1, device_id={"seq": z - 1}, device_id_type=MESH)

    weights = []
    denoms = []
    for p in range(pairs):
        logits = None
        for ri in range(2):
            r = 2 * p + ri
            lhs = []
            for kv in range(2):
                row = ri * 2 + kv
                block = jnp.where(
                    sub == row,
                    queries[r : r + 1, (2 * kv) * PAGE : (2 * kv + 1) * PAGE],
                    jnp.where(
                        sub == 4 + row,
                        queries[r : r + 1, (2 * kv + 1) * PAGE : (2 * kv + 2) * PAGE],
                        0.0,
                    ),
                )
                lhs.append(block)
            lhs = jnp.concatenate(lhs, axis=1).astype(jnp.bfloat16)
            copies[r].wait()
            keys = jnp.concatenate([kbuf[r, 0], kbuf[r, 1]], axis=1)
            term = lax.dot_general(
                lhs, keys, (((1,), (1,)), ((), ())), preferred_element_type=jnp.float32
            )
            logits = term if logits is None else logits + term
        table = rows_of(pt_vec[2 * p : 2 * p + 1, :], pt_vec[2 * p + 1 : 2 * p + 2, :])
        length = rows_of(len_ref[2 * p], len_ref[2 * p + 1])
        total = None
        tiles = []
        for s in range(slots):
            hit = jnp.where(table == z * slots + s, lane, 0).astype(jnp.float32)
            logical = jnp.sum(hit, axis=1, keepdims=True).astype(jnp.int32)
            live = logical * PAGE + lane < length
            tile = logits[:, s * PAGE : (s + 1) * PAGE]
            capped = softcap * jnp.tanh(tile * query_scale / softcap)
            tile = jnp.where(live, jnp.exp(capped - softcap), 0.0)
            gath[p, z * slots + s] = tile
            tiles.append(tile)
            total = tile if total is None else total + tile
        weights.append(jnp.concatenate(tiles, axis=1).astype(jnp.bfloat16))
        denoms.append(jnp.sum(total, axis=1, keepdims=True))

        if p == 0:
            greeted()

        @pl.when(direct)
        def _():
            for c in range(CUTS):
                chunk_copy(z, p, c, own_send.at[p, c], target).start()

    part[z, 2] = jnp.where(lane == 0, denoms[0], denoms[1])
    for p in range(pairs):
        numer = jnp.zeros((8, PAGE), jnp.float32)
        for ri in range(2):
            r = 2 * p + ri
            v_copies[r].wait()
            values = jnp.concatenate([vbuf[r, 0], vbuf[r, 1]], axis=1)
            out = jnp.dot(weights[p], values, preferred_element_type=jnp.float32)
            for kv in range(2):
                mine = lax.rem(sub, 4) == ri * 2 + kv
                numer = jnp.where(mine, out[:, kv * PAGE : (kv + 1) * PAGE], numer)
        part[z, p] = numer

    @pl.when(direct)
    def _():
        part_copy(z, own_part_send, target).start()

    def arrive(src):
        for p in range(pairs):
            for c in range(CUTS):
                chunk_copy(src, p, c, fwd_send.at[src, p, c], 0).wait_recv()
        part_copy(src, fwd_part_send.at[src], 0).wait_recv()

    def relay(src, goes_to, arrives, sends, chunk_sems, part_sems):
        for p in range(pairs):
            for c in range(CUTS):

                @pl.when(arrives)
                def _():
                    chunk_copy(src, p, c, fwd_send.at[src, p, c], 0).wait_recv()

                @pl.when(sends)
                def _():
                    chunk_copy(src, p, c, chunk_sems.at[src, p, c], goes_to).start()

        @pl.when(arrives)
        def _():
            part_copy(src, fwd_part_send.at[src], 0).wait_recv()

        @pl.when(sends)
        def _():
            part_copy(src, part_sems.at[src], goes_to).start()

    half = n // 2
    yes = z >= 0
    no = z < 0

    def down(src, carry):
        sends = jnp.logical_and(z < n - 1, src != z + 1)
        relay(src, z + 1, src != z, sends, fwd_send, fwd_part_send)
        return carry

    def up(src, carry):
        relay(src, 0, no, yes, zero_send, zero_part_send)
        return carry

    def both(src, carry):
        down(src, carry)

        @pl.when(hub)
        def _():
            up(src, carry)

        return carry

    @pl.when(passes_on)
    def _():
        pl.semaphore_wait(ready, 1)

    @pl.when(jnp.logical_not(edge))
    def _():
        lax.fori_loop(1, half, down, 0)

        @pl.when(hub)
        def _():
            pl.semaphore_wait(zero_ready, 1)
            lax.fori_loop(1, half, up, 0)

        lax.fori_loop(half, n - TAIL, both, 0)
        down(0, 0)
        lax.fori_loop(n - TAIL, n, down, 0)

    @pl.when(edge)
    def _():
        def hand_on(src, carry):
            relay(src, 1, yes, yes, fwd_send, fwd_part_send)
            return carry

        def take(src, carry):
            arrive(src)
            return carry

        lax.fori_loop(n - TAIL, n, hand_on, 0)
        lax.fori_loop(1, n - TAIL, take, 0)

    den = jnp.sum(part[:, 2], axis=0)
    for p in range(pairs):
        inv = 1.0 / jnp.sum(jnp.where(lane == p, den, 0.0), axis=1, keepdims=True)
        numer = jnp.sum(part[:, p], axis=0) * inv
        for ri in range(2):
            r = 2 * p + ri
            for kv in range(2):
                for g in range(2):
                    row = g * 4 + ri * 2 + kv
                    h = 2 * kv + g
                    att32[r : r + 1, h * PAGE : (h + 1) * PAGE] = numer[row : row + 1]
        keep = jnp.zeros((4, slots), jnp.float32)
        for j in range(slots):
            even = gath[p, pt_ref[2 * p, z * slots + j]]
            odd = gath[p, pt_ref[2 * p + 1, z * slots + j]]
            tile = rows_of(even, odd) * inv
            mass = tile[:4] + tile[4:]
            for ri in range(2):
                mass_ref[2 * p + ri, :, j * PAGE : (j + 1) * PAGE] = mass[2 * ri : 2 * ri + 2]
            page = jnp.sum(mass, axis=1, keepdims=True)
            column = lax.broadcasted_iota(jnp.int32, (4, slots), 1)
            keep = jnp.where(column == j, page, keep)
        for ri in range(2):
            r = 2 * p + ri
            which = lax.broadcasted_iota(jnp.int32, (2, slots), 0)
            thr = jnp.where(which == 0, thr_ref[0, r], thr_ref[1, r]).astype(jnp.float32)
            keep_ref[r] = jnp.minimum(1.0, quanta * keep[2 * ri : 2 * ri + 2] / thr)
    att_ref[...] = att32[...].astype(att_ref.dtype)

    @pl.when(direct)
    def _():
        for p in range(pairs):
            for c in range(CUTS):
                chunk_copy(z, p, c, own_send.at[p, c], 0).wait_send()
        part_copy(z, own_part_send, 0).wait_send()

    def left(src, chunk_sems, part_sems):
        for p in range(pairs):
            for c in range(CUTS):
                chunk_copy(src, p, c, chunk_sems.at[src, p, c], 0).wait_send()
        part_copy(src, part_sems.at[src], 0).wait_send()

    def drain(src, carry):
        sent = jnp.where(edge, src >= n - TAIL, jnp.logical_and(z < n - 1, src != z + 1))

        @pl.when(sent)
        def _():
            left(src, fwd_send, fwd_part_send)

        @pl.when(jnp.logical_and(hub, jnp.logical_and(src > 0, src < n - TAIL)))
        def _():
            left(src, zero_send, zero_part_send)

        return carry

    lax.fori_loop(0, n, drain, 0)


def put_out(*refs):
    count = len(refs) // 2
    sems = refs[-1]
    ins, outs = refs[:count], refs[count : 2 * count]
    moves = [pltpu.make_async_copy(i, o, sems.at[k]) for k, (i, o) in enumerate(zip(ins, outs))]
    for move in moves:
        move.start()
    for move in moves:
        move.wait()


def shards(queries, k_cache, v_cache, page_table, lengths, keep_threshold):
    n = lax.axis_size("seq")
    requests, kv_local, tok_local, head_size = k_cache.shape
    slots = tok_local // PAGE
    vmem = pl.BlockSpec(memory_space=pltpu.VMEM)
    smem = pl.BlockSpec(memory_space=pltpu.SMEM)
    hbm = pl.BlockSpec(memory_space=pl.ANY)
    dma = pltpu.SemaphoreType.DMA
    pairs = requests // 2
    results = (
        (queries.shape, jnp.bfloat16),
        ((requests, kv_local, tok_local), jnp.float32),
        ((requests, kv_local, slots), jnp.float32),
    )
    held = pl.pallas_call(
        attend,
        out_shape=tuple(pltpu.VMEM(*result) for result in results),
        in_specs=[vmem, vmem, smem, smem, smem, hbm, hbm],
        out_specs=(vmem, vmem, vmem),
        scratch_shapes=[
            pltpu.VMEM(k_cache.shape, k_cache.dtype),
            pltpu.VMEM(v_cache.shape, v_cache.dtype),
            pltpu.VMEM((pairs, n * slots, 8, PAGE), jnp.float32),
            pltpu.VMEM((n, 3, 8, PAGE), jnp.float32),
            pltpu.VMEM(queries.shape, jnp.float32),
            dma((requests,)), dma((requests,)),
            dma((n, pairs, CUTS)), dma((n,)),
            dma((pairs, CUTS)), dma,
            dma((n, pairs, CUTS)), dma((n,)),
            dma((n, pairs, CUTS)), dma((n,)),
            pltpu.SemaphoreType.REGULAR, pltpu.SemaphoreType.REGULAR,
        ],
        compiler_params=pltpu.CompilerParams(collective_id=0, has_side_effects=True),
    )(queries, page_table, page_table, lengths, keep_threshold.T, k_cache, v_cache)
    return pl.pallas_call(
        put_out,
        out_shape=tuple(jax.ShapeDtypeStruct(*result) for result in results),
        in_specs=[vmem] * 3,
        out_specs=(hbm, hbm, hbm),
        scratch_shapes=[dma((3,))],
    )(*(pltpu.with_memory_space_constraint(h, pltpu.VMEM) for h in held))


def solution(mesh):
    placed = (
        P(("grp", "rep"), "head"),
        P(("grp", "rep"), "head", "seq", None),
        P(("grp", "rep"), "head", "seq", None),
        P(("grp", "rep"), None),
        P(("grp", "rep")),
        P(("grp", "rep"), "head"),
    )
    return jax.shard_map(
        shards,
        mesh=mesh,
        in_specs=placed,
        out_specs=(
            P(("grp", "rep"), "head"),
            P(("grp", "rep"), "head", "seq"),
            P(("grp", "rep"), "head", "seq"),
        ),
        check_vma=False,
    )
```

```python
import jax
import jax.numpy as jnp
from jax import lax
from jax.experimental import pallas as pl
from jax.experimental.pallas import tpu as pltpu
from jax.sharding import PartitionSpec as P

PAGE = 128
TAIL = 2
CUTS = 2
MESH = pl.DeviceIdType.MESH

softcap = 50.0
query_scale = 1.0 / 12.0
quanta = 65536.0


def attend(
    q_hbm, pt_hbm, len_hbm, thr_hbm, k_hbm, v_hbm,
    att_ref, mass_ref, keep_ref,
    q_ref, pt_vec, pt_ref, len_ref, thr_ref, kbuf, vbuf, gath, att32,
    in_sem, k_sem, v_sem, recv, own_send, far_send, fwd_send, zero_send,
    ready, zero_ready, far_ready,
):
    n = lax.axis_size("seq")
    z = lax.axis_index("seq")
    requests = k_hbm.shape[0]
    pairs = requests // 2
    slots = k_hbm.shape[2] // PAGE
    extra = pairs * slots
    tiles = extra + pairs + 1
    per = slots // CUTS
    pieces = [(c * per, per) for c in range(pairs * CUTS)] + [(extra, pairs + 1)]
    rest = len(pieces) - 1

    mid_at = n // 4
    half = n // 2
    edge = z == 0
    hub = z == 1
    mid = z == mid_at
    bend = z == half - 1
    low_end = jnp.logical_and(z > mid_at, z < half)
    tail = z >= n - TAIL
    follows = z > 1
    passes_on = jnp.logical_and(z > 0, z < n - 1)

    small = [
        pltpu.make_async_copy(src, dst, in_sem.at[i])
        for i, (src, dst) in enumerate(
            [(q_hbm, q_ref), (pt_hbm, pt_vec), (len_hbm, len_ref), (pt_hbm, pt_ref), (thr_hbm, thr_ref)]
        )
    ]
    copies = []
    for r in range(requests):
        if r == 1:
            for copy in small:
                copy.start()
        k_copy = pltpu.make_async_copy(k_hbm.at[r], kbuf.at[r], k_sem.at[r])
        k_copy.start()
        copies.append(k_copy)
    v_copies = []
    for r in range(requests):
        v_copy = pltpu.make_async_copy(v_hbm.at[r], vbuf.at[r], v_sem.at[r])
        v_copy.start()
        v_copies.append(v_copy)

    barrier = pltpu.get_barrier_semaphore()

    def greet(target):
        pl.semaphore_signal(barrier, inc=1, device_id={"seq": target}, device_id_type=MESH)

    @pl.when(hub)
    def _():
        greet(0)
        for other in range(2, n):
            greet(other)

    @pl.when(edge)
    def _():
        for other in range(n - TAIL, n):
            greet(other)

    @pl.when(passes_on)
    def _():
        greet(z + 1)

    @pl.when(mid)
    def _():
        greet(0)
        for other in range(mid_at + 1, half + 1):
            greet(other)

    @pl.when(z == half)
    def _():
        for other in range(half + 1, n):
            greet(other)

    @pl.when(edge)
    def _():
        pl.semaphore_wait(barrier, 2)
        for feeder in (1, mid_at):
            pl.semaphore_signal(
                zero_ready, inc=1, device_id={"seq": feeder}, device_id_type=MESH
            )

    sub = lax.broadcasted_iota(jnp.int32, (8, PAGE), 0)
    lane = lax.broadcasted_iota(jnp.int32, (8, PAGE), 1)
    first = lax.rem(sub, 4) < 2
    for copy in small:
        copy.wait()
    queries = q_ref[...].astype(jnp.float32)

    def rows_of(even, odd):
        return jnp.where(first, even, odd)

    def piece_copy(src, i, send_sem, target):
        block = gath.at[pl.ds(src * tiles + pieces[i][0], pieces[i][1])]
        return pltpu.make_async_remote_copy(
            src_ref=block, dst_ref=block, send_sem=send_sem, recv_sem=recv.at[src, i],
            device_id={"seq": target}, device_id_type=MESH,
        )

    direct = jnp.logical_not(hub)
    target = jnp.where(tail, 0, 1)

    def send_own(i):
        @pl.when(direct)
        def _():
            piece_copy(z, i, own_send, target).start()

    def greeted():
        @pl.when(follows)
        def _():
            more = z > mid_at
            pl.semaphore_wait(barrier, 2 + more.astype(jnp.int32) + tail.astype(jnp.int32))
            pl.semaphore_signal(ready, inc=1, device_id={"seq": z - 1}, device_id_type=MESH)

        @pl.when(z == half)
        def _():
            pl.semaphore_signal(
                far_ready, inc=1, device_id={"seq": mid_at}, device_id_type=MESH
            )

        @pl.when(z == n - TAIL)
        def _():
            pl.semaphore_signal(
                zero_ready, inc=1, device_id={"seq": z - 1}, device_id_type=MESH
            )

    weights = []
    denoms = []
    for p in range(pairs):
        table = rows_of(pt_vec[2 * p : 2 * p + 1, :], pt_vec[2 * p + 1 : 2 * p + 2, :])
        length = rows_of(len_ref[2 * p], len_ref[2 * p + 1])
        lives = []
        for s in range(slots):
            hit = jnp.where(table == z * slots + s, lane, 0).astype(jnp.float32)
            logical = jnp.sum(hit, axis=1, keepdims=True).astype(jnp.int32)
            lives.append(logical * PAGE + lane < length)
        logits = None
        for ri in range(2):
            r = 2 * p + ri
            lhs = []
            for kv in range(2):
                row = ri * 2 + kv
                block = jnp.where(
                    sub == row,
                    queries[r : r + 1, (2 * kv) * PAGE : (2 * kv + 1) * PAGE],
                    jnp.where(
                        sub == 4 + row,
                        queries[r : r + 1, (2 * kv + 1) * PAGE : (2 * kv + 2) * PAGE],
                        0.0,
                    ),
                )
                lhs.append(block)
            lhs = jnp.concatenate(lhs, axis=1).astype(jnp.bfloat16)
            copies[r].wait()
            keys = jnp.concatenate([kbuf[r, 0], kbuf[r, 1]], axis=1)
            term = lax.dot_general(
                lhs, keys, (((1,), (1,)), ((), ())), preferred_element_type=jnp.float32
            )
            logits = term if logits is None else logits + term
        total = None
        parts = []
        for s in range(slots):
            tile = logits[:, s * PAGE : (s + 1) * PAGE]
            capped = softcap * jnp.tanh(tile * query_scale / softcap)
            tile = jnp.where(lives[s], jnp.exp(capped - softcap), 0.0)
            gath[z * tiles + p * slots + s] = tile
            parts.append(tile)
            total = tile if total is None else total + tile
        weights.append(jnp.concatenate(parts, axis=1).astype(jnp.bfloat16))
        denoms.append(jnp.sum(total, axis=1, keepdims=True))
        if p == 0:
            greeted()
        for c in range(CUTS):
            send_own(p * CUTS + c)

    gath[z * tiles + extra + pairs] = jnp.where(lane == 0, denoms[0], denoms[1])
    for p in range(pairs):
        numer = jnp.zeros((8, PAGE), jnp.float32)
        for ri in range(2):
            r = 2 * p + ri
            v_copies[r].wait()
            values = jnp.concatenate([vbuf[r, 0], vbuf[r, 1]], axis=1)
            out = jnp.dot(weights[p], values, preferred_element_type=jnp.float32)
            for kv in range(2):
                mine = lax.rem(sub, 4) == ri * 2 + kv
                numer = jnp.where(mine, out[:, kv * PAGE : (kv + 1) * PAGE], numer)
        gath[z * tiles + extra + p] = numer
    send_own(rest)
    last = z == n - 1
    before_tail = z == n - TAIL - 1
    for when, other in ((last, 1), (low_end, mid_at), (z > half, half), (before_tail, 0)):

        @pl.when(when)
        def _():
            if other == 0:
                pl.semaphore_wait(zero_ready, 1)
            for i in range(len(pieces)):
                piece_copy(z, i, own_send, other).start()

    def each(src, *steps):
        for i in range(len(pieces)):
            for whether, what in steps:

                @pl.when(whether)
                def _():
                    what(i)

    def down(src, up):
        goes = jnp.logical_and(z < n - 1, src != z + 1)
        goes = jnp.logical_and(goes, jnp.logical_or(z != half - 1, jnp.logical_and(src > 0, src < half)))
        goes = jnp.logical_and(
            goes,
            jnp.logical_or(z != mid_at - 1, jnp.logical_or(src < mid_at, src >= half)),
        )
        each(
            src,
            (src != z, lambda i: piece_copy(src, i, fwd_send, 0).wait_recv()),
            (goes, lambda i: piece_copy(src, i, fwd_send, z + 1).start()),
            (up, lambda i: piece_copy(src, i, zero_send, 0).start()),
        )

    def stretch(start, stop, up):
        def one(src, carry):
            down(src, up)
            return carry

        lax.fori_loop(start, stop, one, 0)

    never = z < 0

    @pl.when(jnp.logical_not(edge))
    def _():
        @pl.when(passes_on)
        def _():
            pl.semaphore_wait(ready, 1)

        @pl.when(mid)
        def _():
            pl.semaphore_wait(zero_ready, 1)

        stretch(1, half, mid)

        @pl.when(hub)
        def _():
            pl.semaphore_wait(zero_ready, 1)

        stretch(half, n - TAIL - 1, hub)
        stretch(n - TAIL - 1, n - TAIL, never)

        @pl.when(z < half)
        def _():
            down(0, never)

        @pl.when(mid)
        def _():
            pl.semaphore_wait(far_ready, 1)
            for i in range(len(pieces)):
                piece_copy(0, i, far_send, half).start()

        stretch(n - TAIL, n, never)

        @pl.when(z >= half)
        def _():
            down(0, never)

    @pl.when(edge)
    def _():
        always = z >= 0

        def hand_on(src, carry):
            for i in range(len(pieces)):
                piece_copy(src, i, fwd_send, 0).wait_recv()
                piece_copy(src, i, fwd_send, 1).start()
            return carry

        def take(src, carry):
            each(src, (always, lambda i: piece_copy(src, i, fwd_send, 0).wait_recv()))
            return carry

        lax.fori_loop(n - TAIL, n - 1, hand_on, 0)
        take(n - 1, 0)
        lax.fori_loop(1, n - TAIL, take, 0)

    def over_all(tile):
        return sum(gath[src * tiles + tile] for src in range(n))

    den = over_all(extra + pairs)
    for p in range(pairs):
        inv = 1.0 / jnp.sum(jnp.where(lane == p, den, 0.0), axis=1, keepdims=True)
        numer = over_all(extra + p) * inv
        for ri in range(2):
            r = 2 * p + ri
            for kv in range(2):
                for g in range(2):
                    row = g * 4 + ri * 2 + kv
                    h = 2 * kv + g
                    att32[r : r + 1, h * PAGE : (h + 1) * PAGE] = numer[row : row + 1]
        keep = jnp.zeros((4, slots), jnp.float32)

        def page(r, j):
            slot = pt_ref[r, z * slots + j]
            owner = lax.div(slot, slots)
            return gath[owner * (tiles - slots) + slot + p * slots]

        for j in range(slots):
            tile = rows_of(page(2 * p, j), page(2 * p + 1, j)) * inv
            mass = tile[:4] + tile[4:]
            for ri in range(2):
                mass_ref[2 * p + ri, :, j * PAGE : (j + 1) * PAGE] = mass[2 * ri : 2 * ri + 2]
            column = lax.broadcasted_iota(jnp.int32, (4, slots), 1)
            keep = jnp.where(column == j, jnp.sum(mass, axis=1, keepdims=True), keep)
        for ri in range(2):
            r = 2 * p + ri
            which = lax.broadcasted_iota(jnp.int32, (2, slots), 0)
            thr = jnp.where(which == 0, thr_ref[0, r], thr_ref[1, r]).astype(jnp.float32)
            keep_ref[r] = jnp.minimum(1.0, quanta * keep[2 * ri : 2 * ri + 2] / thr)
    att_ref[...] = att32[...].astype(att_ref.dtype)

    def sent(amount, sem):
        region = gath.at[pl.ds(0, amount)]
        pltpu.make_async_remote_copy(
            src_ref=region, dst_ref=region, send_sem=sem, recv_sem=recv.at[0, 0],
            device_id={"seq": 0}, device_id_type=MESH,
        ).wait_send()

    thrice = jnp.logical_or(last, before_tail)
    twice = jnp.logical_and(jnp.logical_or(low_end, z > half), jnp.logical_not(thrice))
    once = jnp.logical_not(jnp.logical_or(twice, thrice))
    skips = z == mid_at - 1
    others = jnp.logical_not(jnp.logical_or(bend, skips))
    for when, amount, sem in (
        (jnp.logical_and(direct, once), tiles, own_send),
        (twice, 2 * tiles, own_send),
        (thrice, 3 * tiles, own_send),
        (mid, tiles, far_send),
        (edge, (TAIL - 1) * tiles, fwd_send),
        (jnp.logical_and(passes_on, others), (n - 1) * tiles, fwd_send),
        (skips, (n + mid_at - half) * tiles, fwd_send),
        (bend, (half - 1) * tiles, fwd_send),
        (mid, (half - 1) * tiles, zero_send),
        (hub, (n - TAIL - 1 - half) * tiles, zero_send),
    ):

        @pl.when(when)
        def _():
            sent(amount, sem)


def put_out(*refs):
    count = len(refs) // 2
    sems = refs[-1]
    ins, outs = refs[:count], refs[count : 2 * count]
    moves = [pltpu.make_async_copy(i, o, sems.at[k]) for k, (i, o) in enumerate(zip(ins, outs))]
    for move in moves:
        move.start()
    for move in moves:
        move.wait()


def shards(queries, k_cache, v_cache, page_table, lengths, keep_threshold):
    n = lax.axis_size("seq")
    requests, kv_local, tok_local, head_size = k_cache.shape
    slots = tok_local // PAGE
    vmem = pl.BlockSpec(memory_space=pltpu.VMEM)
    hbm = pl.BlockSpec(memory_space=pl.ANY)
    dma = pltpu.SemaphoreType.DMA
    pairs = requests // 2
    results = (
        (queries.shape, jnp.bfloat16),
        ((requests, kv_local, tok_local), jnp.float32),
        ((requests, kv_local, slots), jnp.float32),
    )
    tiles = pairs * slots + pairs + 1
    regular = pltpu.SemaphoreType.REGULAR
    held = pl.pallas_call(
        attend,
        out_shape=tuple(pltpu.VMEM(*result) for result in results),
        in_specs=[hbm] * 6,
        out_specs=(vmem, vmem, vmem),
        scratch_shapes=[
            pltpu.VMEM(queries.shape, queries.dtype),
            pltpu.VMEM(page_table.shape, jnp.int32),
            pltpu.SMEM(page_table.shape, jnp.int32),
            pltpu.SMEM(lengths.shape, jnp.int32),
            pltpu.SMEM(keep_threshold.shape[::-1], jnp.int32),
            pltpu.VMEM(k_cache.shape, k_cache.dtype),
            pltpu.VMEM(v_cache.shape, v_cache.dtype),
            pltpu.VMEM((n * tiles, 8, PAGE), jnp.float32),
            pltpu.VMEM(queries.shape, jnp.float32),
            dma((5,)), dma((requests,)), dma((requests,)),
            dma((n, pairs * CUTS + 1)), dma, dma, dma, dma,
            regular, regular, regular,
        ],
        compiler_params=pltpu.CompilerParams(collective_id=0, has_side_effects=True),
    )(queries, page_table, lengths, keep_threshold.T, k_cache, v_cache)
    return pl.pallas_call(
        put_out,
        out_shape=tuple(jax.ShapeDtypeStruct(*result) for result in results),
        in_specs=[vmem] * 3,
        out_specs=(hbm, hbm, hbm),
        scratch_shapes=[dma((3,))],
    )(*(pltpu.with_memory_space_constraint(h, pltpu.VMEM) for h in held))


def solution(mesh):
    placed = (
        P(("grp", "rep"), "head"),
        P(("grp", "rep"), "head", "seq", None),
        P(("grp", "rep"), "head", "seq", None),
        P(("grp", "rep"), None),
        P(("grp", "rep")),
        P(("grp", "rep"), "head"),
    )
    return jax.shard_map(
        shards,
        mesh=mesh,
        in_specs=placed,
        out_specs=(
            P(("grp", "rep"), "head"),
            P(("grp", "rep"), "head", "seq"),
            P(("grp", "rep"), "head", "seq"),
        ),
        check_vma=False,
    )
```

```python
import jax
import jax.numpy as jnp
from jax import lax
from jax.experimental import pallas as pl
from jax.experimental.pallas import tpu as pltpu
from jax.sharding import PartitionSpec as P

PAGE = 128
TAIL = 3
CUTS = 2
MESH = pl.DeviceIdType.MESH

softcap = 50.0
query_scale = 1.0 / 12.0
quanta = 65536.0


def attend(
    q_hbm, pt_hbm, len_hbm, thr_hbm, k_hbm, v_hbm,
    att_ref, mass_ref, keep_ref,
    q_ref, pt_vec, pt_ref, len_ref, thr_ref, kbuf, vbuf, gath, att32,
    in_sem, k_sem, v_sem, recv, recv_low, own_send, end_send, far_send, fwd_send, zero_send,
    ready, zero_ready, far_ready,
):
    n = lax.axis_size("seq")
    z = lax.axis_index("seq")
    requests = k_hbm.shape[0]
    pairs = requests // 2
    slots = k_hbm.shape[2] // PAGE
    extra = pairs * slots
    tiles = extra + pairs + 1
    per = slots // CUTS
    pieces = [(c * per, per) for c in range(pairs * CUTS)] + [(extra, pairs + 1)]
    rest = len(pieces) - 1

    half = n // 2
    jump_at = half - 2
    column = lax.axis_index("grp") + lax.axis_index("head") + lax.axis_index("rep")
    zero_first = column > 0
    zero_late = column == 0
    edge = z == 0
    hub = z == 1
    bend = z == half - 1
    tail = z >= n - TAIL
    follows = z > 1
    passes_on = jnp.logical_and(z > 0, z < n - 1)

    barrier = pltpu.get_barrier_semaphore()

    def greet(target):
        pl.semaphore_signal(barrier, inc=1, device_id={"seq": target}, device_id_type=MESH)

    @pl.when(edge)
    def _():
        greet(n - 1)

        @pl.when(zero_first)
        def _():
            for other in range(n - TAIL, n - 1):
                greet(other)

    small = [
        pltpu.make_async_copy(src, dst, in_sem.at[i])
        for i, (src, dst) in enumerate(
            [(q_hbm, q_ref), (pt_hbm, pt_vec), (len_hbm, len_ref), (pt_hbm, pt_ref), (thr_hbm, thr_ref)]
        )
    ]
    copies = []
    for r in range(requests):
        if r == 2:
            for copy in small:
                copy.start()
        k_copy = pltpu.make_async_copy(k_hbm.at[r], kbuf.at[r], k_sem.at[r])
        k_copy.start()
        copies.append(k_copy)
    v_copy = pltpu.make_async_copy(v_hbm, vbuf, v_sem)
    v_copy.start()

    @pl.when(hub)
    def _():
        greet(0)
        for other in range(2, n):
            greet(other)

    @pl.when(passes_on)
    def _():
        greet(z + 1)

    @pl.when(z == jump_at)
    def _():
        greet(half)

    @pl.when(z == half)
    def _():
        for other in range(half + 1, n):
            greet(other)

    @pl.when(edge)
    def _():
        pl.semaphore_wait(barrier, 1)

        @pl.when(zero_first)
        def _():
            pl.semaphore_signal(zero_ready, inc=1, device_id={"seq": 1}, device_id_type=MESH)

    sub = lax.broadcasted_iota(jnp.int32, (8, PAGE), 0)
    lane = lax.broadcasted_iota(jnp.int32, (8, PAGE), 1)
    first = lax.rem(sub, 4) < 2
    for copy in small:
        copy.wait()
    queries = q_ref[...].astype(jnp.float32)

    def rows_of(even, odd):
        return jnp.where(first, even, odd)

    def piece_copy(src, i, send_sem, target):
        block = gath.at[pl.ds(src * tiles + pieces[i][0], pieces[i][1])]
        return pltpu.make_async_remote_copy(
            src_ref=block, dst_ref=block, send_sem=send_sem,
            recv_sem=recv.at[jnp.maximum(src - half + 1, 0), i],
            device_id={"seq": target}, device_id_type=MESH,
        )

    coarse = [(0, tiles // 2), (tiles // 2, tiles - tiles // 2)]

    def coarse_copy(src, i, send_sem, target):
        block = gath.at[pl.ds(src * tiles + coarse[i][0], coarse[i][1])]
        return pltpu.make_async_remote_copy(
            src_ref=block, dst_ref=block, send_sem=send_sem, recv_sem=recv_low.at[src, i],
            device_id={"seq": target}, device_id_type=MESH,
        )

    direct = jnp.logical_not(hub)
    low = jnp.logical_and(z > 1, z < half)
    to_zero = jnp.logical_and(tail, zero_first)
    target = jnp.where(to_zero, 0, 1)

    last = z == n - 1
    waits = jnp.logical_and(tail, jnp.logical_not(last))
    goes_on = jnp.logical_or(edge, jnp.logical_and(z >= half, jnp.logical_not(waits)))

    def send_own(i):
        @pl.when(goes_on)
        def _():
            piece_copy(z, i, own_send, target).start()

    def greeted():
        @pl.when(follows)
        def _():
            count = 2
            for more in (z == half, z > half, jnp.logical_or(to_zero, z == n - 1)):
                count = count + more.astype(jnp.int32)
            pl.semaphore_wait(barrier, count)
            pl.semaphore_signal(ready, inc=1, device_id={"seq": z - 1}, device_id_type=MESH)

        @pl.when(z == half)
        def _():
            pl.semaphore_signal(
                far_ready, inc=1, device_id={"seq": jump_at}, device_id_type=MESH
            )

    weights = []
    denoms = []
    for p in range(pairs):
        table = rows_of(pt_vec[2 * p : 2 * p + 1, :], pt_vec[2 * p + 1 : 2 * p + 2, :])
        length = rows_of(len_ref[2 * p], len_ref[2 * p + 1])
        lives = []
        for s in range(slots):
            hit = jnp.where(table == z * slots + s, lane, 0).astype(jnp.float32)
            logical = jnp.sum(hit, axis=1, keepdims=True).astype(jnp.int32)
            lives.append(logical * PAGE + lane < length)
        logits = None
        for ri in range(2):
            r = 2 * p + ri
            lhs = []
            for kv in range(2):
                row = ri * 2 + kv
                block = jnp.where(
                    sub == row,
                    queries[r : r + 1, (2 * kv) * PAGE : (2 * kv + 1) * PAGE],
                    jnp.where(
                        sub == 4 + row,
                        queries[r : r + 1, (2 * kv + 1) * PAGE : (2 * kv + 2) * PAGE],
                        0.0,
                    ),
                )
                lhs.append(block)
            lhs = jnp.concatenate(lhs, axis=1).astype(jnp.bfloat16)
            copies[r].wait()
            keys = jnp.concatenate([kbuf[r, 0], kbuf[r, 1]], axis=1)
            term = lax.dot_general(
                lhs, keys, (((1,), (1,)), ((), ())), preferred_element_type=jnp.float32
            )
            logits = term if logits is None else logits + term
        total = None
        parts = []
        for s in range(slots):
            tile = logits[:, s * PAGE : (s + 1) * PAGE]
            capped = softcap * jnp.tanh(tile * query_scale / softcap)
            tile = jnp.where(lives[s], jnp.exp(capped - softcap), 0.0)
            gath[z * tiles + p * slots + s] = tile
            parts.append(tile)
            total = tile if total is None else total + tile
        weights.append(jnp.concatenate(parts, axis=1).astype(jnp.bfloat16))
        denoms.append(jnp.sum(total, axis=1, keepdims=True))
        if p == 0:

            @pl.when(jnp.logical_not(waits))
            def _():
                greeted()

        for c in range(CUTS):
            send_own(p * CUTS + c)

    gath[z * tiles + extra + pairs] = jnp.where(lane == 0, denoms[0], denoms[1])
    v_copy.wait()
    for p in range(pairs):
        numer = jnp.zeros((8, PAGE), jnp.float32)
        for ri in range(2):
            r = 2 * p + ri
            values = jnp.concatenate([vbuf[r, 0], vbuf[r, 1]], axis=1)
            out = jnp.dot(weights[p], values, preferred_element_type=jnp.float32)
            for kv in range(2):
                mine = lax.rem(sub, 4) == ri * 2 + kv
                numer = jnp.where(mine, out[:, kv * PAGE : (kv + 1) * PAGE], numer)
        gath[z * tiles + extra + p] = numer
    send_own(rest)

    @pl.when(waits)
    def _():
        greeted()
        for i in range(len(pieces)):
            piece_copy(z, i, own_send, target).start()

    @pl.when(jnp.logical_and(last, zero_first))
    def _():
        piece_copy(z, rest, end_send, 1).start()

    @pl.when(low)
    def _():
        for i in range(len(coarse)):
            coarse_copy(z, i, own_send, 1).start()

    @pl.when(z > half)
    def _():
        for i in range(len(pieces)):
            piece_copy(z, i, own_send, half).start()

    def down(src, up, lower):
        after = jnp.where(z < n - 1, z + 1, 0)
        goes = jnp.logical_and(jnp.logical_or(z < n - 1, zero_late), src != after)
        goes = jnp.logical_and(
            goes, jnp.logical_or(z != half - 1, jnp.logical_and(src > 0, src < half))
        )
        copy = coarse_copy if lower else piece_copy
        for i in range(len(coarse if lower else pieces)):

            @pl.when(src != z)
            def _():
                copy(src, i, fwd_send, 0).wait_recv()

            @pl.when(goes)
            def _():
                copy(src, i, fwd_send, after).start()

            @pl.when(up)
            def _():
                copy(src, i, zero_send, 0).start()

    def stretch(start, stop, up, lower=False):
        def one(src, carry):
            down(src, up, lower)
            return carry

        lax.fori_loop(start, stop, one, 0)

    never = z < 0

    @pl.when(jnp.logical_not(edge))
    def _():
        @pl.when(passes_on)
        def _():
            pl.semaphore_wait(ready, 1)

        feeds = jnp.logical_and(hub, zero_first)

        @pl.when(feeds)
        def _():
            pl.semaphore_wait(zero_ready, 1)

        @pl.when(z < half)
        def _():
            stretch(1, half, feeds, True)

        stretch(half, n - TAIL, feeds)

        def block_zero():
            down(0, never, False)

            @pl.when(z == jump_at)
            def _():
                pl.semaphore_wait(far_ready, 1)
                for i in range(len(pieces)):
                    piece_copy(0, i, far_send, half).start()

        @pl.when(jnp.logical_and(z < half, zero_first))
        def _():
            block_zero()

        stretch(n - TAIL, n, never)

        @pl.when(jnp.logical_and(z < half, zero_late))
        def _():
            block_zero()

        @pl.when(z >= half)
        def _():
            stretch(1, half, never, True)
            down(0, never, False)

    @pl.when(edge)
    def _():
        def hand_on(src, carry):
            for i in range(len(pieces)):
                piece_copy(src, i, fwd_send, 0).wait_recv()
                if i < rest:
                    piece_copy(src, i, fwd_send, 1).start()
                else:

                    @pl.when(src < n - 1)
                    def _():
                        piece_copy(src, i, fwd_send, 1).start()

            return carry

        def take(src, carry):
            for i in range(len(pieces)):
                piece_copy(src, i, fwd_send, 0).wait_recv()
            return carry

        def take_low(src, carry):
            for i in range(len(coarse)):
                coarse_copy(src, i, fwd_send, 0).wait_recv()
            return carry

        @pl.when(zero_first)
        def _():
            lax.fori_loop(n - TAIL, n, hand_on, 0)

        @pl.when(zero_late)
        def _():
            lax.fori_loop(n - TAIL, n, take, 0)

        lax.fori_loop(1, half, take_low, 0)
        lax.fori_loop(half, n - TAIL, take, 0)

    def over_all(tile):
        return sum(gath[src * tiles + tile] for src in range(n))

    den = over_all(extra + pairs)
    for p in range(pairs):
        inv = 1.0 / jnp.sum(jnp.where(lane == p, den, 0.0), axis=1, keepdims=True)
        numer = over_all(extra + p) * inv
        for ri in range(2):
            r = 2 * p + ri
            for kv in range(2):
                for g in range(2):
                    row = g * 4 + ri * 2 + kv
                    h = 2 * kv + g
                    att32[r : r + 1, h * PAGE : (h + 1) * PAGE] = numer[row : row + 1]
        keep = jnp.zeros((4, slots), jnp.float32)

        def page(r, j):
            slot = pt_ref[r, z * slots + j]
            owner = lax.div(slot, slots)
            return gath[owner * (tiles - slots) + slot + p * slots]

        for j in range(slots):
            tile = rows_of(page(2 * p, j), page(2 * p + 1, j)) * inv
            mass = tile[:4] + tile[4:]
            for ri in range(2):
                mass_ref[2 * p + ri, :, j * PAGE : (j + 1) * PAGE] = mass[2 * ri : 2 * ri + 2]
            column = lax.broadcasted_iota(jnp.int32, (4, slots), 1)
            keep = jnp.where(column == j, jnp.sum(mass, axis=1, keepdims=True), keep)
        for ri in range(2):
            r = 2 * p + ri
            which = lax.broadcasted_iota(jnp.int32, (2, slots), 0)
            thr = jnp.where(which == 0, thr_ref[0, r], thr_ref[1, r]).astype(jnp.float32)
            keep_ref[r] = jnp.minimum(1.0, quanta * keep[2 * ri : 2 * ri + 2] / thr)
    att_ref[...] = att32[...].astype(att_ref.dtype)

    def sent(amount, sem):
        region = gath.at[pl.ds(0, amount)]
        pltpu.make_async_remote_copy(
            src_ref=region, dst_ref=region, send_sem=sem, recv_sem=recv.at[0, 0],
            device_id={"seq": 0}, device_id_type=MESH,
        ).wait_send()

    twice = z > half
    once = jnp.logical_not(twice)
    for when, amount, sem in (
        (jnp.logical_and(direct, once), tiles, own_send),
        (twice, 2 * tiles, own_send),
        (jnp.logical_and(last, zero_first), pairs + 1, end_send),
        (z == jump_at, tiles, far_send),
        (jnp.logical_and(edge, zero_first), TAIL * tiles - pairs - 1, fwd_send),
        (jnp.logical_and(passes_on, jnp.logical_not(bend)), (n - 1) * tiles, fwd_send),
        (bend, (half - 1) * tiles, fwd_send),
        (jnp.logical_and(last, zero_late), (n - 1) * tiles, fwd_send),
        (jnp.logical_and(hub, zero_first), (n - TAIL - 1) * tiles, zero_send),
    ):

        @pl.when(when)
        def _():
            sent(amount, sem)


def put_out(*refs):
    count = len(refs) // 2
    sems = refs[-1]
    ins, outs = refs[:count], refs[count : 2 * count]
    moves = [pltpu.make_async_copy(i, o, sems.at[k]) for k, (i, o) in enumerate(zip(ins, outs))]
    for move in moves:
        move.start()
    for move in moves:
        move.wait()


def shards(queries, k_cache, v_cache, page_table, lengths, keep_threshold):
    n = lax.axis_size("seq")
    requests, kv_local, tok_local, head_size = k_cache.shape
    slots = tok_local // PAGE
    vmem = pl.BlockSpec(memory_space=pltpu.VMEM)
    hbm = pl.BlockSpec(memory_space=pl.ANY)
    dma = pltpu.SemaphoreType.DMA
    pairs = requests // 2
    results = (
        (queries.shape, jnp.bfloat16),
        ((requests, kv_local, tok_local), jnp.float32),
        ((requests, kv_local, slots), jnp.float32),
    )
    tiles = pairs * slots + pairs + 1
    regular = pltpu.SemaphoreType.REGULAR
    held = pl.pallas_call(
        attend,
        out_shape=tuple(pltpu.VMEM(*result) for result in results),
        in_specs=[hbm] * 6,
        out_specs=(vmem, vmem, vmem),
        scratch_shapes=[
            pltpu.VMEM(queries.shape, queries.dtype),
            pltpu.VMEM(page_table.shape, jnp.int32),
            pltpu.SMEM(page_table.shape, jnp.int32),
            pltpu.SMEM(lengths.shape, jnp.int32),
            pltpu.SMEM(keep_threshold.shape[::-1], jnp.int32),
            pltpu.VMEM(k_cache.shape, k_cache.dtype),
            pltpu.VMEM(v_cache.shape, v_cache.dtype),
            pltpu.VMEM((n * tiles, 8, PAGE), jnp.float32),
            pltpu.VMEM(queries.shape, jnp.float32),
            dma((5,)), dma((requests,)), dma,
            dma((n // 2 + 1, pairs * CUTS + 1)), dma((n // 2, 2)), dma, dma, dma, dma, dma,
            regular, regular, regular,
        ],
        compiler_params=pltpu.CompilerParams(collective_id=0, has_side_effects=True),
    )(queries, page_table, lengths, keep_threshold.T, k_cache, v_cache)
    return pl.pallas_call(
        put_out,
        out_shape=tuple(jax.ShapeDtypeStruct(*result) for result in results),
        in_specs=[vmem] * 3,
        out_specs=(hbm, hbm, hbm),
        scratch_shapes=[dma((3,))],
    )(*(pltpu.with_memory_space_constraint(h, pltpu.VMEM) for h in held))


def solution(mesh):
    placed = (
        P(("grp", "rep"), "head"),
        P(("grp", "rep"), "head", "seq", None),
        P(("grp", "rep"), "head", "seq", None),
        P(("grp", "rep"), None),
        P(("grp", "rep")),
        P(("grp", "rep"), "head"),
    )
    return jax.shard_map(
        shards,
        mesh=mesh,
        in_specs=placed,
        out_specs=(
            P(("grp", "rep"), "head"),
            P(("grp", "rep"), "head", "seq"),
            P(("grp", "rep"), "head", "seq"),
        ),
        check_vma=False,
    )
```

```python
import jax
import jax.numpy as jnp
from jax import lax
from jax.experimental import pallas as pl
from jax.experimental.pallas import tpu as pltpu
from jax.sharding import PartitionSpec as P

PAGE = 128
TAIL = 3
CUTS = 2
HANDED = 3
MESH = pl.DeviceIdType.MESH

softcap = 50.0
query_scale = 1.0 / 12.0
quanta = 65536.0


def attend(
    q_hbm, pt_hbm, len_hbm, thr_hbm, k_hbm, v_hbm,
    att_ref, mass_ref, keep_ref,
    q_ref, pt_vec, pt_ref, len_ref, thr_ref, kbuf, vbuf, gath, att32,
    in_sem, k_sem, v_sem, recv, recv_low, own_send, end_send, far_send, fwd_send, zero_send,
    ready, zero_ready, far_ready,
):
    n = lax.axis_size("seq")
    z = lax.axis_index("seq")
    requests = k_hbm.shape[0]
    pairs = requests // 2
    slots = k_hbm.shape[2] // PAGE
    extra = pairs * slots
    tiles = extra + pairs + 1
    per = slots // CUTS
    pieces = [(c * per, per) for c in range(pairs * CUTS)] + [(extra, pairs + 1)]
    rest = len(pieces) - 1
    direct_end = tiles - HANDED * per

    half = n // 2
    jump_at = half - 2
    column = lax.axis_index("grp") + lax.axis_index("head") + lax.axis_index("rep")
    zero_first = column > 0
    zero_late = column == 0
    edge = z == 0
    hub = z == 1
    bend = z == half - 1
    tail = z >= n - TAIL
    follows = z > 1
    passes_on = jnp.logical_and(z > 0, z < n - 1)

    barrier = pltpu.get_barrier_semaphore()

    def greet(target):
        pl.semaphore_signal(barrier, inc=1, device_id={"seq": target}, device_id_type=MESH)

    @pl.when(edge)
    def _():
        greet(n - 1)

        @pl.when(zero_first)
        def _():
            for other in range(n - TAIL, n - 1):
                greet(other)

    small = [
        pltpu.make_async_copy(src, dst, in_sem.at[i])
        for i, (src, dst) in enumerate(
            [(q_hbm, q_ref), (pt_hbm, pt_vec), (len_hbm, len_ref), (pt_hbm, pt_ref), (thr_hbm, thr_ref)]
        )
    ]
    copies = []
    for p in range(pairs):
        two = pl.ds(2 * p, 2)
        k_copy = pltpu.make_async_copy(k_hbm.at[two], kbuf.at[two], k_sem.at[p])
        k_copy.start()
        copies.append(k_copy)
        if p == 0:
            for copy in small:
                copy.start()
    v_copy = pltpu.make_async_copy(v_hbm, vbuf, v_sem)
    v_copy.start()

    @pl.when(hub)
    def _():
        greet(0)
        for other in range(2, n):
            greet(other)

    @pl.when(passes_on)
    def _():
        greet(z + 1)

    @pl.when(z == jump_at)
    def _():
        greet(half)

    @pl.when(z == half)
    def _():
        for other in range(half + 1, n):
            greet(other)

    @pl.when(edge)
    def _():
        pl.semaphore_wait(barrier, 1)

        @pl.when(zero_first)
        def _():
            pl.semaphore_signal(zero_ready, inc=1, device_id={"seq": 1}, device_id_type=MESH)

    sub = lax.broadcasted_iota(jnp.int32, (8, PAGE), 0)
    lane = lax.broadcasted_iota(jnp.int32, (8, PAGE), 1)
    first = lax.rem(sub, 4) < 2
    for copy in small:
        copy.wait()
    queries = q_ref[...].astype(jnp.float32)

    def rows_of(even, odd):
        return jnp.where(first, even, odd)

    def piece_copy(src, i, send_sem, target):
        block = gath.at[pl.ds(src * tiles + pieces[i][0], pieces[i][1])]
        return pltpu.make_async_remote_copy(
            src_ref=block, dst_ref=block, send_sem=send_sem,
            recv_sem=recv.at[jnp.maximum(src - half + 1, 0), i],
            device_id={"seq": target}, device_id_type=MESH,
        )

    coarse = [(0, tiles // 2), (tiles // 2, tiles - tiles // 2)]

    def coarse_copy(src, i, send_sem, target):
        block = gath.at[pl.ds(src * tiles + coarse[i][0], coarse[i][1])]
        return pltpu.make_async_remote_copy(
            src_ref=block, dst_ref=block, send_sem=send_sem, recv_sem=recv_low.at[src, i],
            device_id={"seq": target}, device_id_type=MESH,
        )

    direct = jnp.logical_not(hub)
    low = jnp.logical_and(z > 1, z < half)
    to_zero = jnp.logical_and(tail, zero_first)
    target = jnp.where(to_zero, 0, 1)

    last = z == n - 1
    goes_on = jnp.logical_or(edge, z >= half)

    def send_own(i):
        @pl.when(goes_on)
        def _():
            piece_copy(z, i, own_send, target).start()

    def greeted():
        @pl.when(follows)
        def _():
            count = 2
            for more in (z == half, z > half, jnp.logical_or(to_zero, z == n - 1)):
                count = count + more.astype(jnp.int32)
            pl.semaphore_wait(barrier, count)
            pl.semaphore_signal(ready, inc=1, device_id={"seq": z - 1}, device_id_type=MESH)

        @pl.when(z == half)
        def _():
            pl.semaphore_signal(
                far_ready, inc=1, device_id={"seq": jump_at}, device_id_type=MESH
            )

    weights = []
    denoms = []
    for p in range(pairs):
        table = rows_of(pt_vec[2 * p : 2 * p + 1, :], pt_vec[2 * p + 1 : 2 * p + 2, :])
        length = rows_of(len_ref[2 * p], len_ref[2 * p + 1])
        lives = []
        for s in range(slots):
            hit = jnp.where(table == z * slots + s, lane, 0).astype(jnp.float32)
            logical = jnp.sum(hit, axis=1, keepdims=True).astype(jnp.int32)
            lives.append(logical * PAGE + lane < length)
        logits = None
        for ri in range(2):
            r = 2 * p + ri
            lhs = []
            for kv in range(2):
                row = ri * 2 + kv
                block = jnp.where(
                    sub == row,
                    queries[r : r + 1, (2 * kv) * PAGE : (2 * kv + 1) * PAGE],
                    jnp.where(
                        sub == 4 + row,
                        queries[r : r + 1, (2 * kv + 1) * PAGE : (2 * kv + 2) * PAGE],
                        0.0,
                    ),
                )
                lhs.append(block)
            lhs = jnp.concatenate(lhs, axis=1).astype(jnp.bfloat16)
            if ri == 0:
                copies[p].wait()
            keys = jnp.concatenate([kbuf[r, 0], kbuf[r, 1]], axis=1)
            term = lax.dot_general(
                lhs, keys, (((1,), (1,)), ((), ())), preferred_element_type=jnp.float32
            )
            logits = term if logits is None else logits + term
        total = None
        parts = []
        for s in range(slots):
            tile = logits[:, s * PAGE : (s + 1) * PAGE]
            capped = softcap * jnp.tanh(tile * query_scale / softcap)
            tile = jnp.where(lives[s], jnp.exp(capped - softcap), 0.0)
            gath[z * tiles + p * slots + s] = tile
            parts.append(tile)
            total = tile if total is None else total + tile
        weights.append(jnp.concatenate(parts, axis=1).astype(jnp.bfloat16))
        denoms.append(jnp.sum(total, axis=1, keepdims=True))
        if p == 0:
            greeted()

        for c in range(CUTS):
            send_own(p * CUTS + c)

    gath[z * tiles + extra + pairs] = jnp.where(lane == 0, denoms[0], denoms[1])
    v_copy.wait()
    for p in range(pairs):
        numer = jnp.zeros((8, PAGE), jnp.float32)
        for ri in range(2):
            r = 2 * p + ri
            values = jnp.concatenate([vbuf[r, 0], vbuf[r, 1]], axis=1)
            out = jnp.dot(weights[p], values, preferred_element_type=jnp.float32)
            for kv in range(2):
                mine = lax.rem(sub, 4) == ri * 2 + kv
                numer = jnp.where(mine, out[:, kv * PAGE : (kv + 1) * PAGE], numer)
        gath[z * tiles + extra + p] = numer
    send_own(rest)

    @pl.when(jnp.logical_and(last, zero_first))
    def _():
        for i in range(HANDED, len(pieces)):
            piece_copy(z, i, end_send, 1).start()

    @pl.when(low)
    def _():
        for i in range(len(coarse)):
            coarse_copy(z, i, own_send, 1).start()

    @pl.when(z > half)
    def _():
        for i in range(len(pieces)):
            piece_copy(z, i, own_send, half).start()

    def down(src, up, lower):
        after = jnp.where(z < n - 1, z + 1, 0)
        goes = jnp.logical_and(jnp.logical_or(z < n - 1, zero_late), src != after)
        goes = jnp.logical_and(
            goes, jnp.logical_or(z != half - 1, jnp.logical_and(src > 0, src < half))
        )
        copy = coarse_copy if lower else piece_copy
        for i in range(len(coarse if lower else pieces)):

            @pl.when(src != z)
            def _():
                copy(src, i, fwd_send, 0).wait_recv()

            @pl.when(goes)
            def _():
                copy(src, i, fwd_send, after).start()

            @pl.when(up)
            def _():
                copy(src, i, zero_send, 0).start()

    def stretch(start, stop, up, lower=False):
        def one(src, carry):
            down(src, up, lower)
            return carry

        lax.fori_loop(start, stop, one, 0)

    never = z < 0

    @pl.when(jnp.logical_not(edge))
    def _():
        @pl.when(passes_on)
        def _():
            pl.semaphore_wait(ready, 1)

        feeds = jnp.logical_and(hub, zero_first)

        @pl.when(feeds)
        def _():
            pl.semaphore_wait(zero_ready, 1)

        @pl.when(z < half)
        def _():
            stretch(1, half, feeds, True)

        stretch(half, n - TAIL, feeds)

        def block_zero():
            down(0, never, False)

            @pl.when(z == jump_at)
            def _():
                pl.semaphore_wait(far_ready, 1)
                for i in range(len(pieces)):
                    piece_copy(0, i, far_send, half).start()

        @pl.when(jnp.logical_and(z < half, zero_first))
        def _():
            block_zero()

        stretch(n - TAIL, n, never)

        @pl.when(jnp.logical_and(z < half, zero_late))
        def _():
            block_zero()

        @pl.when(z >= half)
        def _():
            stretch(1, half, never, True)
            down(0, never, False)

    @pl.when(edge)
    def _():
        def hand_on(src, carry):
            for i in range(len(pieces)):
                piece_copy(src, i, fwd_send, 0).wait_recv()
                if i < HANDED:
                    piece_copy(src, i, fwd_send, 1).start()
                else:

                    @pl.when(src < n - 1)
                    def _():
                        piece_copy(src, i, fwd_send, 1).start()

            return carry

        def take(src, carry):
            for i in range(len(pieces)):
                piece_copy(src, i, fwd_send, 0).wait_recv()
            return carry

        def take_low(src, carry):
            for i in range(len(coarse)):
                coarse_copy(src, i, fwd_send, 0).wait_recv()
            return carry

        @pl.when(zero_first)
        def _():
            lax.fori_loop(n - TAIL, n, hand_on, 0)

        @pl.when(zero_late)
        def _():
            lax.fori_loop(n - TAIL, n, take, 0)

        lax.fori_loop(1, half, take_low, 0)
        lax.fori_loop(half, n - TAIL, take, 0)

    def over_all(tile):
        return sum(gath[src * tiles + tile] for src in range(n))

    den = over_all(extra + pairs)
    for p in range(pairs):
        inv = 1.0 / jnp.sum(jnp.where(lane == p, den, 0.0), axis=1, keepdims=True)
        numer = over_all(extra + p) * inv
        for ri in range(2):
            r = 2 * p + ri
            for kv in range(2):
                for g in range(2):
                    row = g * 4 + ri * 2 + kv
                    h = 2 * kv + g
                    att32[r : r + 1, h * PAGE : (h + 1) * PAGE] = numer[row : row + 1]
        keep = jnp.zeros((4, slots), jnp.float32)

        def page(r, j):
            slot = pt_ref[r, z * slots + j]
            owner = lax.div(slot, slots)
            return gath[owner * (tiles - slots) + slot + p * slots]

        for j in range(slots):
            tile = rows_of(page(2 * p, j), page(2 * p + 1, j)) * inv
            mass = tile[:4] + tile[4:]
            for ri in range(2):
                mass_ref[2 * p + ri, :, j * PAGE : (j + 1) * PAGE] = mass[2 * ri : 2 * ri + 2]
            column = lax.broadcasted_iota(jnp.int32, (4, slots), 1)
            keep = jnp.where(column == j, jnp.sum(mass, axis=1, keepdims=True), keep)
        for ri in range(2):
            r = 2 * p + ri
            which = lax.broadcasted_iota(jnp.int32, (2, slots), 0)
            thr = jnp.where(which == 0, thr_ref[0, r], thr_ref[1, r]).astype(jnp.float32)
            keep_ref[r] = jnp.minimum(1.0, quanta * keep[2 * ri : 2 * ri + 2] / thr)
    att_ref[...] = att32[...].astype(att_ref.dtype)

    def sent(amount, sem):
        region = gath.at[pl.ds(0, amount)]
        pltpu.make_async_remote_copy(
            src_ref=region, dst_ref=region, send_sem=sem, recv_sem=recv.at[0, 0],
            device_id={"seq": 0}, device_id_type=MESH,
        ).wait_send()

    twice = z > half
    once = jnp.logical_not(twice)
    for when, amount, sem in (
        (jnp.logical_and(direct, once), tiles, own_send),
        (twice, 2 * tiles, own_send),
        (jnp.logical_and(last, zero_first), direct_end, end_send),
        (z == jump_at, tiles, far_send),
        (jnp.logical_and(edge, zero_first), TAIL * tiles - direct_end, fwd_send),
        (jnp.logical_and(passes_on, jnp.logical_not(bend)), (n - 1) * tiles, fwd_send),
        (bend, (half - 1) * tiles, fwd_send),
        (jnp.logical_and(last, zero_late), (n - 1) * tiles, fwd_send),
        (jnp.logical_and(hub, zero_first), (n - TAIL - 1) * tiles, zero_send),
    ):

        @pl.when(when)
        def _():
            sent(amount, sem)


def put_out(*refs):
    count = len(refs) // 2
    sems = refs[-1]
    ins, outs = refs[:count], refs[count : 2 * count]
    moves = [pltpu.make_async_copy(i, o, sems.at[k]) for k, (i, o) in enumerate(zip(ins, outs))]
    for move in moves:
        move.start()
    for move in moves:
        move.wait()


def shards(queries, k_cache, v_cache, page_table, lengths, keep_threshold):
    n = lax.axis_size("seq")
    requests, kv_local, tok_local, head_size = k_cache.shape
    slots = tok_local // PAGE
    vmem = pl.BlockSpec(memory_space=pltpu.VMEM)
    hbm = pl.BlockSpec(memory_space=pl.ANY)
    dma = pltpu.SemaphoreType.DMA
    pairs = requests // 2
    results = (
        (queries.shape, jnp.bfloat16),
        ((requests, kv_local, tok_local), jnp.float32),
        ((requests, kv_local, slots), jnp.float32),
    )
    tiles = pairs * slots + pairs + 1
    regular = pltpu.SemaphoreType.REGULAR
    held = pl.pallas_call(
        attend,
        out_shape=tuple(pltpu.VMEM(*result) for result in results),
        in_specs=[hbm] * 6,
        out_specs=(vmem, vmem, vmem),
        scratch_shapes=[
            pltpu.VMEM(queries.shape, queries.dtype),
            pltpu.VMEM(page_table.shape, jnp.int32),
            pltpu.SMEM(page_table.shape, jnp.int32),
            pltpu.SMEM(lengths.shape, jnp.int32),
            pltpu.SMEM(keep_threshold.shape[::-1], jnp.int32),
            pltpu.VMEM(k_cache.shape, k_cache.dtype),
            pltpu.VMEM(v_cache.shape, v_cache.dtype),
            pltpu.VMEM((n * tiles, 8, PAGE), jnp.float32),
            pltpu.VMEM(queries.shape, jnp.float32),
            dma((5,)), dma((pairs,)), dma,
            dma((n // 2 + 1, pairs * CUTS + 1)), dma((n // 2, 2)), dma, dma, dma, dma, dma,
            regular, regular, regular,
        ],
        compiler_params=pltpu.CompilerParams(collective_id=0, has_side_effects=True),
    )(queries, page_table, lengths, keep_threshold.T, k_cache, v_cache)
    return pl.pallas_call(
        put_out,
        out_shape=tuple(jax.ShapeDtypeStruct(*result) for result in results),
        in_specs=[vmem] * 3,
        out_specs=(hbm, hbm, hbm),
        scratch_shapes=[dma((3,))],
    )(*(pltpu.with_memory_space_constraint(h, pltpu.VMEM) for h in held))


def solution(mesh):
    placed = (
        P(("grp", "rep"), "head"),
        P(("grp", "rep"), "head", "seq", None),
        P(("grp", "rep"), "head", "seq", None),
        P(("grp", "rep"), None),
        P(("grp", "rep")),
        P(("grp", "rep"), "head"),
    )
    return jax.shard_map(
        shards,
        mesh=mesh,
        in_specs=placed,
        out_specs=(
            P(("grp", "rep"), "head"),
            P(("grp", "rep"), "head", "seq"),
            P(("grp", "rep"), "head", "seq"),
        ),
        check_vma=False,
    )
```
